32 devices in a mesh: kvp: 16 (over z, y, x), tp: 2 (over core).
Axes of the slice: x: 2, y: 2, z: 4, core: 2. Of those that a mesh axis runs over, the one named last changes fastest.
Arguments:
- queries: bfloat16 [8, 8192], P(None, 'tp'), may hold values from -12 to 12
- key_pool: bfloat16 [512, 64, 1024], P('kvp', None, 'tp'), may hold values from -5 to 5
- value_pool: bfloat16 [512, 64, 1024], P('kvp', None, 'tp'), may hold values from -5 to 5
- block_table: int32 [16, 32], P('kvp'), may hold values from 0 to 31, each once within a row
- lengths: int32 [8], replicated, may hold values from 1 to 4096, 20480 in all
- residual_in: float32 [8, 8192], P(None, 'kvp'), may hold values from -12 to 12
- out_weight: bfloat16 [8192, 8192], P('tp', 'kvp'), may hold values from -0.0625 to 0.0625
- norm_gain: bfloat16 [8192], P('kvp'), may hold values from 0.25 to 1.75
- gate_weight: bfloat16 [8192, 28672], P('kvp', 'tp'), may hold values from -0.0625 to 0.0625
- up_weight: bfloat16 [8192, 28672], P('kvp', 'tp'), may hold values from -0.0625 to 0.0625
- down_weight: bfloat16 [28672, 8192], P('tp', 'kvp'), may hold values from -0.03125 to 0.03125
Outputs:
- attended: bfloat16 [8, 8192], P(None, 'tp')
- layer_out: float32 [8, 8192], P(None, 'kvp')
The draws below stay inside these ranges and needn't reach their ends.
Inputs may be any that keep to these rules, and one draw needn't show every extreme that they name: Row s is a permutation of 0 to 31; the page of request b's block j in KV shard s is s * 32 + block_table[s, b * 4 + j]. The lengths sum to 20480 and the longest is exactly 4096.
All inputs are finite; a program needn't handle non-finite values.
Results may differ from the reference program's by a relative error of at most 0.0056.
Values may be sent and summed in bfloat16 or wider, within the bound.
A program may use at most 128 MiB of HBM per device.

```python
import math
import jax
import jax.numpy as jnp
import numpy as np
from jax import lax

D = 8192
H = 64
KVH = 8
HD = 128
FF = 28672
BATCH = 8
PAGE = 64
SHARDS = 16
CTX = 4096
POOL_DEV = 32
PAGES = 512


def draw_queries(key, part):
    shape = (BATCH, H * HD)
    drawn = jnp.clip(2.5 * jax.random.normal(jax.random.fold_in(key, 11), shape, jnp.float32), -12.0, 12.0)
    return drawn.astype(jnp.bfloat16)


def draw_key_pool(key, part):
    shape = (PAGES, PAGE, KVH * HD)
    drawn = jnp.clip(jax.random.normal(jax.random.fold_in(key, 13), shape, jnp.float32), -5.0, 5.0)
    return drawn.astype(jnp.bfloat16)


def draw_residual_in(key, part):
    width = D // SHARDS
    levels = jax.random.uniform(jax.random.fold_in(key, 31), (BATCH, SHARDS), jnp.float32, math.log(0.2), math.log(3.0))
    scales = jnp.repeat(jnp.exp(levels), width, axis=1)
    base = jnp.clip(jax.random.normal(jax.random.fold_in(key, 37), (BATCH, D), jnp.float32), -4.0, 4.0)
    return (base * scales).astype(jnp.float32)


def level_of(stream_key, shape, split, low, largest):
    level = 1.0
    for axis_at, parts in split:
        steps = jax.random.uniform(jax.random.fold_in(jax.random.fold_in(stream_key, 6), axis_at), (parts,), jnp.float32, low / len(split), largest / len(split))
        level = level * jnp.repeat(jnp.exp(steps), shape[axis_at] // parts).reshape((-1,) + (1,) * (len(shape) - 1 - axis_at))
    return level


def split_up(number_of, total, limit, lean):
    loads = [(1 << 20) // math.isqrt(grade ** lean) + 1 for grade in range(2, number_of + 1)]
    rest, holding = total - limit - (number_of - 1), [1] * (number_of - 1)
    while rest > 0:
        movable = [i for i in range(number_of - 1) if holding[i] < limit]
        whole, budget = sum([loads[i] for i in movable]), rest
        for i in movable:
            extra = min(limit - holding[i], max(1, budget * loads[i] // whole), rest)
            holding[i] = holding[i] + extra
            rest = rest - extra
    return np.array([limit] + holding)


def uneven_parts(rng, number_of, total, limit, skew):
    if number_of == 2:
        one = jax.random.randint(rng, (), max(1, total - limit), min(limit, total - 1) + 1)
        return jnp.stack([one, total - one])
    sizes = jnp.asarray(split_up(number_of, total, limit, skew), jnp.int32)
    pairs = (number_of - 1) // 2
    donor, receiver = sizes[1:1 + 2 * pairs:2], sizes[2:2 + 2 * pairs:2]
    slack = jnp.minimum(donor - 1, limit - receiver)
    shifted = jax.random.randint(jax.random.fold_in(rng, 1), (pairs,), 0, 1 << 20) % (slack + 1)
    sizes = sizes.at[1:1 + 2 * pairs:2].set(donor - shifted).at[2:2 + 2 * pairs:2].set(receiver + shifted)
    return sizes[jax.random.permutation(jax.random.fold_in(rng, 2), number_of)]


def centred(key, dims, scale, bound, shards=(), kind=jnp.bfloat16):
    gain = level_of(key, dims, shards, -0.22, 0.18) if shards else 1.0
    values = jax.random.normal(key, dims, jnp.float32) * scale * gain
    return jnp.minimum(jnp.maximum(values, -bound), bound).astype(kind)


def setup_inputs(seed: int = 0) -> dict:
    keys = jax.random.split(jax.random.key(seed), 12)
    return {
        "queries": draw_queries(jax.random.fold_in(keys[11], 71), 0),
        "key_pool": draw_key_pool(jax.random.fold_in(keys[11], 71), 0),
        "value_pool": centred(keys[2], (PAGES, PAGE, KVH * HD), 1.0, 5.0, ((0, 16), (2, 2))),
        "block_table": jax.vmap(lambda own: jax.random.permutation(own, POOL_DEV))(jax.random.split(keys[3], SHARDS)).reshape((SHARDS, POOL_DEV)).astype(jnp.int32),
        "lengths": uneven_parts(keys[4], BATCH, BATCH * CTX * 5 // 8, CTX, 1).astype(jnp.int32),
        "residual_in": draw_residual_in(jax.random.fold_in(keys[11], 71), 0),
        "out_weight": centred(keys[6], (H * HD, D), (H * HD) ** -0.5, 0.0625, ((0, 2), (1, 16))),
        "norm_gain": jnp.clip(1.0 + 0.15 * jax.random.normal(keys[7], (D,), jnp.float32), 0.25, 1.75).astype(jnp.bfloat16),
        "gate_weight": centred(keys[8], (D, FF), D ** -0.5, 0.0625, ((0, 16), (1, 2))),
        "up_weight": centred(keys[9], (D, FF), D ** -0.5, 0.0625, ((0, 16), (1, 2))),
        "down_weight": centred(keys[10], (FF, D), FF ** -0.5, 0.03125, ((0, 2), (1, 16))),
    }


def reference(queries, key_pool, value_pool, block_table, lengths, residual_in, out_weight, norm_gain, gate_weight, up_weight, down_weight):
    requests = queries.shape[0]
    shard_count = block_table.shape[0]
    pool_size = block_table.shape[1]
    blocks = pool_size // requests
    page_rows = key_pool.shape[1]
    context = shard_count * blocks * page_rows
    group_size = H // KVH
    offsets = (jnp.arange(shard_count, dtype=jnp.int32) * pool_size)[:, None]
    page_ids = (block_table.astype(jnp.int32) + offsets).reshape(shard_count, requests, blocks)
    page_ids = jnp.transpose(page_ids, (1, 0, 2))
    positions = jnp.arange(context, dtype=jnp.int32)

    def attend_request(request):
        wanted = page_ids[request].reshape(-1)
        key_rows = key_pool[wanted].reshape(context, KVH, HD).astype(jnp.float32)
        value_rows = value_pool[wanted].reshape(context, KVH, HD).astype(jnp.float32)
        query_heads = queries[request].reshape(KVH, group_size, HD).astype(jnp.float32)
        scores = jnp.einsum('kgd,tkd->kgt', query_heads, key_rows) * HD ** (-0.5)
        is_live = positions < lengths[request]
        masked = jnp.where(is_live, scores, -1e+30)
        row_peak = lax.optimization_barrier(jnp.max(masked, axis=-1, keepdims=True))
        weights = jnp.where(is_live, jnp.exp(masked - row_peak), 0.0)
        weight_sum = lax.optimization_barrier(jnp.sum(weights, axis=-1))
        rounded = lax.optimization_barrier(weights.astype(jnp.bfloat16)).astype(jnp.float32)
        out_sum = jnp.einsum('kgt,tkd->kgd', rounded, value_rows)
        return (out_sum / weight_sum[..., None]).reshape(H * HD)
    attended = lax.map(attend_request, jnp.arange(requests, dtype=jnp.int32)).astype(jnp.bfloat16)
    mixed = residual_in + jnp.dot(attended, out_weight, preferred_element_type=jnp.float32)
    inv_rms = lax.rsqrt(lax.optimization_barrier(jnp.sum(mixed * mixed, axis=1, keepdims=True)) / D + 0.1)
    normed = (mixed * inv_rms * norm_gain.astype(jnp.float32)).astype(jnp.bfloat16)
    gate_part = jnp.dot(normed, gate_weight, preferred_element_type=jnp.float32)
    up_part = jnp.dot(normed, up_weight, preferred_element_type=jnp.float32)
    hidden = (jax.nn.silu(gate_part) * up_part).astype(jnp.bfloat16)
    layer_out = mixed + jnp.dot(hidden, down_weight, preferred_element_type=jnp.float32)
    return (attended, layer_out)
```

```python
import functools
import jax
import jax.numpy as jnp
from jax import lax
from jax.experimental import pallas as pl
from jax.experimental.pallas import tpu as pltpu
from jax.sharding import PartitionSpec as P

D = 8192
HD = 128


def merged(part, axis, combine):
    gathered = jax.tree.map(lambda a: lax.all_gather(a, axis), part)

    def take(source):
        return jax.tree.map(lambda a: lax.dynamic_index_in_dim(a, source, 0, False), gathered)

    return lax.fori_loop(
        1, lax.axis_size(axis), lambda source, state: combine(state, take(source)), take(0)
    )


def combine(earlier, later):
    peak_early, sum_early, out_early = earlier
    peak_late, sum_late, out_late = later
    row_peak = jnp.maximum(peak_early, peak_late)
    factor_early = jnp.exp(peak_early - row_peak)
    factor_late = jnp.exp(peak_late - row_peak)
    weight_sum = sum_early * factor_early + sum_late * factor_late
    out_sum = out_early * factor_early[..., None] + out_late * factor_late[..., None]
    return (row_peak, weight_sum, out_sum)


def plain_body(
    queries,
    key_pool,
    value_pool,
    block_table,
    lengths,
    residual_in,
    out_weight,
    norm_gain,
    gate_weight,
    up_weight,
    down_weight,
):
    requests = queries.shape[0]
    kv_local = key_pool.shape[2] // HD
    heads_local = queries.shape[1] // HD
    group_size = heads_local // kv_local
    blocks = block_table.shape[1] // requests
    shard_span = blocks * key_pool.shape[1]
    shard_index = lax.axis_index("kvp")
    page_ids = block_table[0].reshape(requests, blocks)
    key_rows = key_pool[page_ids].reshape(requests, shard_span, kv_local, HD)
    value_rows = value_pool[page_ids].reshape(requests, shard_span, kv_local, HD)
    query_heads = queries.reshape(requests, kv_local, group_size, HD)
    scores = jnp.einsum(
        "bkgd,btkd->bkgt", query_heads, key_rows, preferred_element_type=jnp.float32
    ) * HD ** (-0.5)
    positions = shard_index * shard_span + jnp.arange(shard_span, dtype=jnp.int32)
    is_live = (positions[None, :] < lengths[:, None])[:, None, None, :]
    masked = jnp.where(is_live, scores, -1e30)
    row_peak = jnp.max(masked, axis=-1)
    weights = jnp.where(is_live, jnp.exp(masked - row_peak[..., None]), 0.0)
    weight_sum = jnp.sum(weights, axis=-1).reshape(requests, heads_local)
    rounded = weights.astype(jnp.bfloat16)
    out_sum = jnp.einsum("bkgt,btkd->bkgd", rounded, value_rows, preferred_element_type=jnp.float32)
    out_sum = out_sum.reshape(requests, heads_local, HD)
    row_peak = row_peak.reshape(requests, heads_local)
    row_peak, weight_sum, out_sum = merged((row_peak, weight_sum, out_sum), "kvp", combine)
    attended = (
        (out_sum / weight_sum[..., None]).astype(jnp.bfloat16).reshape(requests, heads_local * HD)
    )
    projected = jnp.dot(attended, out_weight, preferred_element_type=jnp.float32)
    mixed = residual_in + lax.psum(projected, "tp")
    squares = lax.psum(jnp.sum(mixed * mixed, axis=1), "kvp")
    inv_rms = lax.rsqrt(squares / D + 0.1)
    normed = (mixed * inv_rms[:, None] * norm_gain.astype(jnp.float32)).astype(jnp.bfloat16)
    gate_part = jnp.dot(normed, gate_weight, preferred_element_type=jnp.float32)
    up_part = jnp.dot(normed, up_weight, preferred_element_type=jnp.float32)
    gate_full, up_full = lax.psum((gate_part, up_part), "kvp")
    hidden = (jax.nn.silu(gate_full) * up_full).astype(jnp.bfloat16)
    down_part = jnp.dot(hidden, down_weight, preferred_element_type=jnp.float32)
    layer_out = mixed + lax.psum(down_part, "tp")
    return (attended, layer_out)


def remote(src, dst, send_sem, recv_sem, axis, target):
    return pltpu.make_async_remote_copy(
        src_ref=src,
        dst_ref=dst,
        send_sem=send_sem,
        recv_sem=recv_sem,
        device_id={axis: target},
        device_id_type=pl.DeviceIdType.MESH,
    )


def layer_kernel(
    sizes,
    table,
    lengths,
    q_ref,
    residual,
    gain,
    key_hbm,
    value_hbm,
    out_hbm,
    gate_hbm,
    up_hbm,
    down_hbm,
    attended,
    layer_out,
    keys,
    values,
    out_w,
    gate_w,
    up_w,
    down_w,
    o_send,
    o_recv,
    st_send,
    st_recv,
    att,
    att_rows,
    tp_buf,
    sq,
    gu_send,
    gu_recv,
    gu_own,
    hid,
    kv_sem,
    w_sem,
    gate_sem,
    up_sem,
    o_ss,
    o_rs,
    st_ss,
    st_rs,
    att_ss,
    att_rs,
    tp_ss,
    tp_rs,
    sq_ss,
    sq_rs,
    gu_ss,
    gu_rs,
    hid_ss,
    hid_rs,
):
    n, t, requests, heads, kv_local, blocks, page, rp, chunk = sizes
    me = lax.axis_index("kvp")
    me_t = lax.axis_index("tp")
    group = heads // kv_local
    span = blocks * page
    per_request = heads // rp
    f32, bf16 = jnp.float32, jnp.bfloat16

    def peer(i):
        return lax.rem(me + i, n)

    key_copy = pltpu.make_async_copy(key_hbm, keys, kv_sem.at[0])
    value_copy = pltpu.make_async_copy(value_hbm, values, kv_sem.at[1])
    key_copy.start()
    value_copy.start()

    barrier = pltpu.get_barrier_semaphore()
    for i in range(1, n):
        pl.semaphore_signal(
            barrier, inc=1, device_id={"kvp": peer(i)}, device_id_type=pl.DeviceIdType.MESH
        )
    for i in range(1, t):
        pl.semaphore_signal(
            barrier,
            inc=1,
            device_id={"tp": lax.rem(me_t + i, t)},
            device_id_type=pl.DeviceIdType.MESH,
        )

    def gate_copy(i):
        columns = pl.ds(pl.multiple_of(peer(i + 1) * chunk, 128), chunk)
        return pltpu.make_async_copy(gate_hbm.at[:, columns], gate_w.at[i], gate_sem.at[i])

    def up_copy(i):
        columns = pl.ds(pl.multiple_of(peer(i + 1) * chunk, 128), chunk)
        return pltpu.make_async_copy(up_hbm.at[:, columns], up_w.at[i], up_sem.at[i])

    out_copy = pltpu.make_async_copy(out_hbm, out_w, w_sem.at[0])
    down_copy = pltpu.make_async_copy(down_hbm, down_w, w_sem.at[1])
    key_copy.wait()
    value_copy.wait()
    out_copy.start()

    @pl.loop(0, n)
    def _(i):
        gate_copy(i).start()
        up_copy(i).start()

    down_copy.start()
    pl.semaphore_wait(barrier, n - 1 + t - 1)

    row_h = lax.broadcasted_iota(jnp.int32, (heads, kv_local * HD), 0) // group
    lane_k = lax.broadcasted_iota(jnp.int32, (heads, kv_local * HD), 1) // HD
    on_block = row_h == lane_k
    offsets = lax.broadcasted_iota(jnp.int32, (heads, span), 1)
    lane = lax.broadcasted_iota(jnp.int32, (rp, HD), 1)
    row = lax.broadcasted_iota(jnp.int32, (rp, HD), 0)
    first = me // per_request

    def o_copy(target, source):
        return remote(
            o_send.at[target], o_recv.at[source], o_ss.at[target], o_rs.at[source], "kvp", target
        )

    def st_copy(target, source):
        return remote(
            st_send.at[target], st_recv.at[source], st_ss.at[target], st_rs.at[source], "kvp", target
        )

    @pl.loop(0, requests)
    def _(i):
        b = lax.rem(first + i + 1, requests)
        pages = [table[0, b * blocks + j] for j in range(blocks)]
        key_rows = jnp.concatenate([keys[p] for p in pages], axis=0)
        value_rows = jnp.concatenate([values[p] for p in pages], axis=0)
        query = jnp.concatenate([q_ref[b]] * kv_local, axis=1)
        query = jnp.where(on_block, query, 0.0).astype(bf16)
        scores = lax.dot_general(
            query, key_rows, (((1,), (1,)), ((), ())), preferred_element_type=f32
        ) * HD ** (-0.5)
        live = me * span + offsets < lengths[b]
        masked = jnp.where(live, scores, -1e30)
        peak = jnp.max(masked, axis=1, keepdims=True)
        weights = jnp.where(live, jnp.exp(masked - peak), 0.0)
        total = jnp.sum(weights, axis=1, keepdims=True)
        wide = jnp.dot(weights.astype(bf16), value_rows, preferred_element_type=f32)
        wide = jnp.where(on_block, wide, 0.0)
        out = wide[:, :HD]
        for k in range(1, kv_local):
            out = out + wide[:, k * HD : (k + 1) * HD]
        out = out.astype(bf16)
        for c in range(per_request):
            target = b * per_request + c
            rows = slice(c * rp, (c + 1) * rp)
            stats = jnp.where(lane == row, peak[rows], 0.0)
            stats = jnp.where(lane == row + rp, total[rows], stats)
            stats = jnp.sum(stats, axis=0, keepdims=True)

            @pl.when(target == me)
            def _():
                o_recv[me] = out[rows]
                st_recv[me] = stats

            @pl.when(target != me)
            def _():
                o_send[target] = out[rows]
                st_send[target] = stats
                o_copy(target, me).start()
                st_copy(target, me).start()

    @pl.loop(1, n)
    def _(i):
        o_copy(me, peer(i)).wait_recv()
        st_copy(me, peer(i)).wait_recv()

    peaks, totals = [], []
    for s in range(n):
        stats = jnp.broadcast_to(st_recv[s], (rp, HD))
        peaks.append(jnp.sum(jnp.where(lane == row, stats, 0.0), axis=1, keepdims=True))
        totals.append(jnp.sum(jnp.where(lane == row + rp, stats, 0.0), axis=1, keepdims=True))
    top = functools.reduce(jnp.maximum, peaks)
    weight_sum = jnp.zeros((rp, 1), f32)
    out_sum = jnp.zeros((rp, HD), f32)
    for s in range(n):
        factor = jnp.exp(peaks[s] - top)
        weight_sum = weight_sum + totals[s] * factor
        out_sum = out_sum + o_recv[s].astype(f32) * factor
    att[me] = (out_sum / weight_sum).astype(bf16)

    def att_copy(target, source):
        return remote(
            att.at[source], att.at[source], att_ss.at[target], att_rs.at[source], "kvp", target
        )

    @pl.loop(1, n)
    def _(i):
        att_copy(peer(i), me).start()

    out_copy.wait()

    @pl.loop(1, n)
    def _(i):
        att_copy(me, peer(i)).wait_recv()

    for s in range(n):
        att_rows[s * rp : (s + 1) * rp, :] = att[s].astype(f32)
    whole = jnp.concatenate(
        [att_rows[pl.ds(h, requests, stride=heads), :] for h in range(heads)], axis=1
    ).astype(bf16)
    attended[...] = whole

    def over_tp(which, part):
        def tp_copy(target, source):
            return remote(
                tp_buf.at[which, source],
                tp_buf.at[which, source],
                tp_ss.at[which, target],
                tp_rs.at[which, source],
                "tp",
                target,
            )

        tp_buf[which, me_t] = part
        for i in range(1, t):
            tp_copy(lax.rem(me_t + i, t), me_t).start()
        for i in range(1, t):
            tp_copy(me_t, lax.rem(me_t + i, t)).wait_recv()
        total = tp_buf[which, 0]
        for s in range(1, t):
            total = total + tp_buf[which, s]
        for i in range(1, t):
            tp_copy(lax.rem(me_t + i, t), me_t).wait_send()
        return total

    projected = jnp.dot(whole, out_w[...], preferred_element_type=f32)
    mixed = residual[...] + over_tp(0, projected)

    squares = jnp.sum(mixed * mixed, axis=1, keepdims=True)
    sq[me] = jnp.broadcast_to(squares, (requests, HD))

    def sq_copy(target, source):
        return remote(
            sq.at[source], sq.at[source], sq_ss.at[target], sq_rs.at[source], "kvp", target
        )

    @pl.loop(1, n)
    def _(i):
        sq_copy(peer(i), me).start()

    scaled = (mixed * gain[...].astype(f32)).astype(bf16)
    layer_out[...] = mixed

    def gu_copy(target, source):
        return remote(
            gu_send.at[target], gu_recv.at[source], gu_ss.at[target], gu_rs.at[source], "kvp", target
        )

    def gate_up(i):
        gate_copy(i).wait()
        up_copy(i).wait()
        gate = jnp.dot(scaled, gate_w[i], preferred_element_type=f32)
        up = jnp.dot(scaled, up_w[i], preferred_element_type=f32)
        return jnp.concatenate([gate, up], axis=0)

    @pl.loop(0, n - 1)
    def _(i):
        target = peer(i + 1)
        gu_send[target] = gate_up(i).astype(bf16)
        gu_copy(target, me).start()

    gu_own[...] = gate_up(n - 1)

    @pl.loop(1, n)
    def _(i):
        sq_copy(me, peer(i)).wait_recv()

    squares = sq[0]
    for s in range(1, n):
        squares = squares + sq[s]
    inv_rms = lax.rsqrt(squares[:, :1] / (n * residual.shape[1]) + 0.1)

    @pl.loop(1, n)
    def _(i):
        source = lax.rem(me + n - i, n)
        gu_copy(me, source).wait_recv()
        gu_own[...] += gu_recv[source].astype(f32)

    gate = gu_own[:requests, :] * inv_rms
    up = gu_own[requests:, :] * inv_rms
    hid[me] = (gate / (1.0 + jnp.exp(-gate)) * up).astype(bf16)

    def hid_copy(target, source):
        return remote(
            hid.at[source], hid.at[source], hid_ss.at[target], hid_rs.at[source], "kvp", target
        )

    @pl.loop(1, n)
    def _(i):
        hid_copy(peer(i), me).start()

    down_copy.wait()

    def down_step(i, acc):
        source = lax.rem(me + n - i, n)
        hid_copy(me, source).wait_recv()
        return acc + jnp.dot(hid[source], down_w[source], preferred_element_type=f32)

    acc = jnp.dot(hid[me], down_w[me], preferred_element_type=f32)
    acc = lax.fori_loop(1, n, down_step, acc)
    layer_out[...] = layer_out[...] + over_tp(1, acc)

    @pl.loop(1, n)
    def _(i):
        target = peer(i)
        o_copy(target, me).wait_send()
        st_copy(target, me).wait_send()
        att_copy(target, me).wait_send()
        sq_copy(target, me).wait_send()
        gu_copy(target, me).wait_send()
        hid_copy(target, me).wait_send()


def kernel_body(
    queries,
    key_pool,
    value_pool,
    block_table,
    lengths,
    residual_in,
    out_weight,
    norm_gain,
    gate_weight,
    up_weight,
    down_weight,
):
    n, t = lax.axis_size("kvp"), lax.axis_size("tp")
    requests = queries.shape[0]
    heads = queries.shape[1] // HD
    kv_local = key_pool.shape[2] // HD
    blocks = block_table.shape[1] // requests
    page = key_pool.shape[1]
    rp = requests * heads // n
    width, hidden = gate_weight.shape
    chunk = hidden // n
    sizes = (n, t, requests, heads, kv_local, blocks, page, rp, chunk)
    f32, bf16 = jnp.float32, jnp.bfloat16
    vmem = pl.BlockSpec(memory_space=pltpu.VMEM)
    smem = pl.BlockSpec(memory_space=pltpu.SMEM)
    hbm = pl.BlockSpec(memory_space=pl.ANY)
    dma = pltpu.SemaphoreType.DMA
    return pl.pallas_call(
        functools.partial(layer_kernel, sizes),
        out_shape=(
            jax.ShapeDtypeStruct(queries.shape, bf16),
            jax.ShapeDtypeStruct(residual_in.shape, f32),
        ),
        in_specs=[smem, smem, vmem, vmem, vmem, hbm, hbm, hbm, hbm, hbm, hbm],
        out_specs=(vmem, vmem),
        scratch_shapes=[
            pltpu.VMEM(key_pool.shape, bf16),
            pltpu.VMEM(value_pool.shape, bf16),
            pltpu.VMEM(out_weight.shape, bf16),
            pltpu.VMEM((n, width, chunk), bf16),
            pltpu.VMEM((n, width, chunk), bf16),
            pltpu.VMEM((n, chunk, width), bf16),
            pltpu.VMEM((n, rp, HD), bf16),
            pltpu.VMEM((n, rp, HD), bf16),
            pltpu.VMEM((n, 1, HD), f32),
            pltpu.VMEM((n, 1, HD), f32),
            pltpu.VMEM((n, rp, HD), bf16),
            pltpu.VMEM((n * rp, HD), f32),
            pltpu.VMEM((2, t, requests, width), f32),
            pltpu.VMEM((n, requests, HD), f32),
            pltpu.VMEM((n, 2 * requests, chunk), bf16),
            pltpu.VMEM((n, 2 * requests, chunk), bf16),
            pltpu.VMEM((2 * requests, chunk), f32),
            pltpu.VMEM((n, requests, chunk), bf16),
            dma((2,)),
            dma((2,)),
            dma((n,)),
            dma((n,)),
            dma((n,)),
            dma((n,)),
            dma((n,)),
            dma((n,)),
            dma((n,)),
            dma((n,)),
            dma((2, t)),
            dma((2, t)),
            dma((n,)),
            dma((n,)),
            dma((n,)),
            dma((n,)),
            dma((n,)),
            dma((n,)),
        ],
        compiler_params=pltpu.CompilerParams(
            collective_id=0, has_side_effects=True, vmem_limit_bytes=60 * 1024 * 1024
        ),
    )(
        block_table,
        lengths,
        queries.reshape(requests, heads, HD).astype(f32),
        residual_in,
        norm_gain.reshape(1, width),
        key_pool,
        value_pool,
        out_weight,
        gate_weight,
        up_weight,
        down_weight.reshape(n, chunk, width),
    )


def body(*arrays):
    queries, gate_weight = arrays[0], arrays[8]
    n = lax.axis_size("kvp")
    requests = queries.shape[0]
    heads = queries.shape[1] // HD
    hidden = gate_weight.shape[1]
    rp = requests * heads // n
    tiled = rp % 16 == 0 and heads % rp == 0 and 2 * rp <= HD
    tiled = tiled and requests * heads % n == 0 and hidden % (n * HD) == 0
    return (kernel_body if tiled else plain_body)(*arrays)


def solution(mesh):
    return jax.shard_map(
        body,
        mesh=mesh,
        in_specs=(
            P(None, "tp"),
            P("kvp", None, "tp"),
            P("kvp", None, "tp"),
            P("kvp", None),
            P(),
            P(None, "kvp"),
            P("tp", "kvp"),
            P("kvp"),
            P("kvp", "tp"),
            P("kvp", "tp"),
            P("tp", "kvp"),
        ),
        out_specs=(P(None, "tp"), P(None, "kvp")),
        check_vma=False,
    )
```
